256 devices in a mesh: bank: 64 (over z, y, x_lo), ens: 4 (over x_hi, core).
Axes of the slice: x: 4 (x_hi: 2, x_lo: 2; x = x_hi * 2 + x_lo), y: 4, z: 8, core: 2. Of those that a mesh axis runs over, the one named last changes fastest.
Arguments:
- item_ids: int32 [8192, 2], P(('ens', 'bank')), parts along dimension 0, may hold values from 0 to 16383
- large_table: bfloat16 [65536, 256], P(('ens', 'bank')), parts along dimension 0, may hold values from -6 to 6
- dense_part: float32 [8192, 256], P(('ens', 'bank')), parts along dimension 0, may hold values from -6 to 6
- small_ids: int32 [8192], P(('ens', 'bank')), parts along dimension 0, may hold values from 0 to 127
- small_table: bfloat16 [512, 256], P(('ens', 'bank')), parts along dimension 0, may hold values from -6 to 6
- scale_ids: int32 [8192], P(('ens', 'bank')), parts along dimension 0, may hold values from 0 to 127
Outputs:
- features: float32 [8192, 256], P(('ens', 'bank')), parts along dimension 0
The draws below stay inside these ranges and needn't reach their ends.
There are 4 independent parts, one for each index of `ens`. The reference program is written for one: setup_inputs(seed, part) draws one part's arguments, and reference() takes and returns one part's arrays. A program takes and returns all parts, laid end to end along the dimension named above; each array names one. Nothing has to cross between parts.
All inputs are finite; a program needn't handle non-finite values.
Results may differ from the reference program's by a relative error of at most 0.0003.
Values may be sent and summed in bfloat16 or wider, within the bound.
A program may use at most 64 MiB of HBM per device.

```python
import math
import jax
import jax.numpy as jnp
import numpy as np
from jax import lax

EXAMPLES = 2048
FEATURES = 256
PICKS = 2
BIG_ROWS = 16384
SMALL_ROWS = 128


def place_ends(result, own_key, least, high):
    dims = result.shape
    index_at = [jax.random.randint(jax.random.fold_in(own_key, axis), (), 0, dims[axis]) for axis in range(len(dims))]
    result = result.at[tuple(index_at)].set(least)
    longest = dims.index(max(dims))
    index_at[longest] = (index_at[longest] + 1) % dims[longest]
    return result.at[tuple(index_at)].set(high)


def steps_of(own_key, dims, cuts, smallest, largest):
    level = 1.0
    for dim, shards_of in cuts:
        steps = jax.random.uniform(jax.random.fold_in(jax.random.fold_in(own_key, 6), dim), (shards_of,), jnp.float32, smallest / len(cuts), largest / len(cuts))
        level = level * jnp.repeat(jnp.exp(steps), dims[dim] // shards_of).reshape((-1,) + (1,) * (len(dims) - 1 - dim))
    return level


def rank_table(number_of, skew):
    loads = [(1 << 20) // math.isqrt(grade ** skew) + 1 for grade in range(1, number_of + 1)]
    scale = 1 + sum(loads) // (1 << 30)
    return np.cumsum(np.array([max(1, weight // scale) for weight in loads]))


def ranked_ids(own_key, extent, number_of, skew):
    grid = rank_table(number_of, skew)
    ticket = jax.random.randint(jax.random.fold_in(own_key, 1), extent, 0, int(grid[number_of - 1]))
    standing = jnp.searchsorted(jnp.asarray(grid, jnp.int32), ticket, side="right")
    return jax.random.permutation(jax.random.fold_in(own_key, 2), number_of)[standing].astype(jnp.int32)


def gaussian(stream_key, dims, spread, bound, cuts=(), kind=jnp.bfloat16):
    factor_of = steps_of(stream_key, dims, cuts, -0.22, 0.18) if cuts else 1.0
    values = jax.random.normal(stream_key, dims, jnp.float32) * spread * factor_of
    return jnp.minimum(jnp.maximum(values, -bound), bound).astype(kind)


def setup_inputs(seed: int = 0, part: int = 0) -> dict:
    seeds = jax.random.split(jax.random.key(seed), 7)
    part_keys = jax.random.split(jax.random.fold_in(seeds[6], part), 7)
    item_ids = place_ends(ranked_ids(part_keys[0], (EXAMPLES, PICKS), BIG_ROWS, 1), jax.random.fold_in(part_keys[0], 3), 0, BIG_ROWS - 1).astype(jnp.int32)
    large_table = gaussian(part_keys[1], (BIG_ROWS, FEATURES), 1.0, 6.0, ((0, 64),))
    dense_part = gaussian(part_keys[2], (EXAMPLES, FEATURES), 1.0, 6.0, ((0, 64),), jnp.float32)
    small_ids = place_ends(jax.random.randint(part_keys[3], (EXAMPLES,), 0, SMALL_ROWS), jax.random.fold_in(part_keys[3], 1), 0, SMALL_ROWS - 1).astype(jnp.int32)
    small_table = gaussian(part_keys[4], (SMALL_ROWS, FEATURES), 1.0, 6.0, ((0, 64),))
    scale_ids = place_ends(ranked_ids(part_keys[5], (EXAMPLES,), SMALL_ROWS, 1), jax.random.fold_in(part_keys[5], 3), 0, SMALL_ROWS - 1).astype(jnp.int32)
    return {"item_ids": item_ids, "large_table": large_table, "dense_part": dense_part, "small_ids": small_ids, "small_table": small_table, "scale_ids": scale_ids}


def reference(item_ids, large_table, dense_part, small_ids, small_table, scale_ids):
    pooled = lax.optimization_barrier(jnp.sum(large_table[item_ids].astype(jnp.float32), axis=1)) * PICKS ** (-0.5)
    small_rows = small_table[small_ids].astype(jnp.float32)
    dense_part = dense_part * small_table[scale_ids].astype(jnp.float32)
    total = dense_part + pooled * small_rows
    features = total * lax.rsqrt(lax.optimization_barrier(jnp.mean(total * total, axis=-1, keepdims=True)) + 1e-06)
    return features
```

```python
import jax
import jax.numpy as jnp
from jax import lax
from jax.experimental import pallas as pl
from jax.experimental.pallas import tpu as pltpu
from jax.sharding import PartitionSpec as P

PICKS = 2
NZ, NY, NX = 8, 4, 2
Z_ORDER = (4, 3, 5, 2, 6, 1, 7)
MESH = pl.DeviceIdType.MESH


def kernel(
    ids_hbm,
    table_hbm,
    dense_hbm,
    small_ids_hbm,
    scale_ids_hbm,
    small_hbm,
    out_ref,
    tab,
    idb,
    smb,
    dense,
    picks,
    onehot,
    part,
    x_out,
    x_in,
    z_out,
    z_in,
    local_sem,
    y_send,
    y_recv,
    r_send,
    r_recv,
    ids_send,
    ids_recv,
    sm_send,
    sm_recv,
    xx_send,
    xx_recv,
    zz_send,
    zz_recv,
):
    bank = lax.axis_index("bank")
    x = lax.rem(bank, NX)
    y = lax.rem(bank // NX, NY)
    z = bank // (NX * NY)

    def at(dz, dy, flip):
        zz = lax.rem(z + dz, NZ)
        yy = lax.rem(y + dy, NY)
        xx = 1 - x if flip else x
        return (zz * NY + yy) * NX + xx

    def remote(src, dst, send, recv, to):
        return pltpu.make_async_remote_copy(
            src_ref=src,
            dst_ref=dst,
            send_sem=send,
            recv_sem=recv,
            device_id={"bank": to},
            device_id_type=MESH,
        )

    rows = table_hbm.shape[0]
    half = rows // 2
    peers_z = [at(k, 0, False) for k in range(NZ)]
    peers_y = [at(0, k, False) for k in range(NY)]
    peer_x = at(0, 0, True)

    barrier = pltpu.get_barrier_semaphore()
    for to in [peer_x] + peers_y[1:] + peers_z[1:]:
        pl.semaphore_signal(barrier, inc=1, device_id={"bank": to}, device_id_type=MESH)

    loads = [
        pltpu.make_async_copy(table_hbm.at[:, pl.ds(0, 128)], tab.at[0, 0], local_sem.at[0]),
        pltpu.make_async_copy(table_hbm.at[:, pl.ds(128, 128)], tab.at[0, 1], local_sem.at[1]),
        pltpu.make_async_copy(ids_hbm, idb.at[0, 0], local_sem.at[2]),
        pltpu.make_async_copy(small_hbm, smb.at[0, 0, 0], local_sem.at[3]),
        pltpu.make_async_copy(dense_hbm, dense, local_sem.at[4]),
        pltpu.make_async_copy(small_ids_hbm, picks.at[0], local_sem.at[5]),
        pltpu.make_async_copy(scale_ids_hbm, picks.at[1], local_sem.at[6]),
    ]
    for load in loads:
        load.start()
    for load in loads:
        load.wait()
    pl.semaphore_wait(barrier, 1 + (NY - 1) + (NZ - 1))

    sent = []

    def go(copy):
        copy.start()
        sent.append(copy)
        return copy

    ids_x = go(remote(idb.at[0, 0], idb.at[0, 1], ids_send.at[0], ids_recv.at[0], peer_x))
    sm_x = go(remote(smb.at[0, 0, 0], smb.at[0, 0, 1], sm_send.at[0], sm_recv.at[0], peer_x))

    own = {}
    for h in range(2):
        for up, r in ((0, 0), (1, 1), (0, 1), (1, 0)):
            slot, to = (3, peers_y[1]) if up == 0 else (1, peers_y[3])
            piece = pl.ds(r * half, half)
            own[up, h, r] = go(
                remote(
                    tab.at[0, h, piece],
                    tab.at[slot, h, piece],
                    y_send.at[up, h, r],
                    y_recv.at[up, h, r],
                    to,
                )
            )

    ids_x.wait_recv()
    ids_z = [
        go(remote(idb.at[0], idb.at[(NZ - k) % NZ], ids_send.at[k], ids_recv.at[k], peers_z[k]))
        for k in Z_ORDER
    ]
    sm_x.wait_recv()
    sm_z = [
        go(
            remote(
                smb.at[0, 0], smb.at[0, (NZ - k) % NZ], sm_send.at[k], sm_recv.at[k], peers_z[k]
            )
        )
        for k in Z_ORDER
    ]

    relay = {}
    for h in range(2):
        for up in range(2):
            slot, to = (3, peers_y[1]) if up == 0 else (1, peers_y[3])
            own[up, h, up].wait_recv()
            piece = pl.ds(up * half, half)
            relay[up, h] = go(
                remote(
                    tab.at[slot, h, piece],
                    tab.at[2, h, piece],
                    r_send.at[up, h],
                    r_recv.at[up, h],
                    to,
                )
            )

    for copy in ids_z:
        copy.wait_recv()
    examples = idb.shape[-1]
    cols = idb[...].reshape(NZ * NX * PICKS, examples).T
    lane = lax.broadcasted_iota(jnp.int32, (examples, rows), 1)
    for kx in range(NX):
        for kz in range(NZ):
            c = (kz * NX + kx) * PICKS
            d = kx * NZ + kz
            for ky in range(NY):
                base = peers_y[ky] * rows
                first = (cols[:, c : c + 1] - base) == lane
                second = (cols[:, c + 1 : c + 2] - base) == lane
                count = jnp.where(first, 1.0, 0.0) + jnp.where(second, 1.0, 0.0)
                onehot[d * examples : (d + 1) * examples, ky * rows : (ky + 1) * rows] = (
                    count.astype(jnp.bfloat16)
                )

    for copy in sm_z:
        copy.wait_recv()
    sm_y = [
        go(
            remote(
                smb.at[0], smb.at[(NY - k) % NY], sm_send.at[NZ + k], sm_recv.at[NZ + k], peers_y[k]
            )
        )
        for k in (2, 1, 3)
    ]

    block = NZ * examples

    def partial(kx, h):
        total = None
        for ky in (0, 1, 3, 2):
            term = jnp.dot(
                onehot[kx * block : (kx + 1) * block, ky * rows : (ky + 1) * rows],
                tab[ky, h],
                preferred_element_type=jnp.float32,
            )
            total = term if total is None else total + term
        return total.reshape(NZ, examples, 128)

    swap = {}
    for h in range(2):
        own[0, h, 1].wait_recv()
        own[1, h, 0].wait_recv()
        relay[0, h].wait_recv()
        relay[1, h].wait_recv()
        x_out[h] = partial(1, h)
        for k in Z_ORDER + (0,):
            swap[k, h] = go(
                remote(
                    x_out.at[h, k], x_in.at[h, k], xx_send.at[h, k], xx_recv.at[h, k], peer_x
                )
            )
        part[h] = partial(0, h)

    deliver = []
    for h in range(2):
        for k in Z_ORDER:
            swap[k, h].wait_recv()
            z_out[h, k] = part[h, k] + x_in[h, k]
            deliver.append(
                go(
                    remote(
                        z_out.at[h, k],
                        z_in.at[h, (NZ - k) % NZ],
                        zz_send.at[h, k],
                        zz_recv.at[h, k],
                        peers_z[k],
                    )
                )
            )
    for h in range(2):
        swap[0, h].wait_recv()

    for copy in sm_y:
        copy.wait_recv()
    small = smb[...].reshape(NY * NZ * NX * 2, 256)
    place = lax.broadcasted_iota(jnp.int32, (examples, NY * NZ * NX * 2), 1)
    sx = lax.rem(place // 2 + x, NX)
    sz = lax.rem(place // (2 * NX) + z, NZ)
    sy = lax.rem(place // (2 * NX * NZ) + y, NY)
    row = ((sz * NY + sy) * NX + sx) * 2 + lax.rem(place, 2)
    pick_cols = picks[...].reshape(2, examples).T
    found = [
        jnp.dot(
            jnp.where(pick_cols[:, i : i + 1] == row, 1.0, 0.0).astype(jnp.bfloat16),
            small,
            preferred_element_type=jnp.float32,
        )
        for i in range(2)
    ]
    scaled = dense[...] * found[1]

    for copy in deliver:
        copy.wait_recv()
    totals = []
    for h in range(2):
        pooled = part[h, 0] + x_in[h, 0]
        for k in range(1, NZ):
            pooled += z_in[h, k]
        pooled = pooled * PICKS ** (-0.5)
        cut = slice(h * 128, (h + 1) * 128)
        totals.append(scaled[:, cut] + pooled * found[0][:, cut])
    power = (
        jnp.sum(totals[0] * totals[0] + totals[1] * totals[1], axis=-1, keepdims=True) / 256.0
    )
    inv = lax.rsqrt(power + 1e-06)
    for h in range(2):
        out_ref[:, h * 128 : (h + 1) * 128] = totals[h] * inv

    for copy in sent:
        copy.wait_send()


def shards(item_ids, large_table, dense_part, small_ids, small_table, scale_ids):
    examples, features = dense_part.shape
    rows = large_table.shape[0]
    any_space = pl.BlockSpec(memory_space=pl.ANY)
    dma = pltpu.SemaphoreType.DMA
    return pl.pallas_call(
        kernel,
        out_shape=jax.ShapeDtypeStruct((examples, features), jnp.float32),
        in_specs=[any_space] * 6,
        out_specs=pl.BlockSpec(memory_space=pltpu.VMEM),
        scratch_shapes=[
            pltpu.VMEM((NY, 2, rows, 128), jnp.bfloat16),
            pltpu.VMEM((NZ, NX, PICKS, examples), jnp.int32),
            pltpu.VMEM((NY, NZ, NX, 2, features), jnp.bfloat16),
            pltpu.VMEM((examples, features), jnp.float32),
            pltpu.VMEM((2, 1, examples), jnp.int32),
            pltpu.VMEM((NX * NZ * examples, NY * rows), jnp.bfloat16),
            pltpu.VMEM((2, NZ, examples, 128), jnp.float32),
            pltpu.VMEM((2, NZ, examples, 128), jnp.float32),
            pltpu.VMEM((2, NZ, examples, 128), jnp.float32),
            pltpu.VMEM((2, NZ, examples, 128), jnp.float32),
            pltpu.VMEM((2, NZ, examples, 128), jnp.float32),
            dma((7,)),
            dma((2, 2, 2)),
            dma((2, 2, 2)),
            dma((2, 2)),
            dma((2, 2)),
            dma((NZ,)),
            dma((NZ,)),
            dma((NZ + NY,)),
            dma((NZ + NY,)),
            dma((2, NZ)),
            dma((2, NZ)),
            dma((2, NZ)),
            dma((2, NZ)),
        ],
        compiler_params=pltpu.CompilerParams(collective_id=0, has_side_effects=True),
    )(
        item_ids.T,
        large_table,
        dense_part,
        small_ids.reshape(1, examples),
        scale_ids.reshape(1, examples),
        small_table,
    )


def solution(mesh):
    return jax.shard_map(
        shards,
        mesh=mesh,
        in_specs=(
            P(("ens", "bank"), None),
            P(("ens", "bank"), None),
            P(("ens", "bank"), None),
            P(("ens", "bank")),
            P(("ens", "bank"), None),
            P(("ens", "bank")),
        ),
        out_specs=P(("ens", "bank"), None),
        check_vma=False,
    )
```

```python
import jax
import jax.numpy as jnp
from jax import lax
from jax.experimental import pallas as pl
from jax.experimental.pallas import tpu as pltpu
from jax.sharding import PartitionSpec as P

PICKS = 2
NZ, NY, NX = 8, 4, 2
FAR_FIRST = (4, 3, 5, 2, 6, 1, 7, 0)
MESH = pl.DeviceIdType.MESH


def kernel(
    ids_hbm,
    table_hbm,
    dense_hbm,
    small_ids_hbm,
    scale_ids_hbm,
    small_hbm,
    out_ref,
    tab,
    idb,
    smb,
    dense,
    picks,
    onehot,
    part,
    x_out,
    x_in,
    z_out,
    z_in,
    load_sem,
    send_sem,
    recv_sem,
    x_sem,
    up_sem,
    y_sem,
):
    bank = lax.axis_index("bank")
    x = lax.rem(bank, NX)
    y = lax.rem(bank // NX, NY)
    z = bank // (NX * NY)

    def at(dz, dy, flip):
        zz = lax.rem(z + dz, NZ)
        yy = lax.rem(y + dy, NY)
        xx = 1 - x if flip else x
        return (zz * NY + yy) * NX + xx

    def remote(src, dst, send, recv, to):
        return pltpu.make_async_remote_copy(
            src_ref=src,
            dst_ref=dst,
            send_sem=send,
            recv_sem=recv,
            device_id={"bank": to},
            device_id_type=MESH,
        )

    rows = table_hbm.shape[0]
    examples = dense_hbm.shape[0]
    column = [(k, 1) for k in FAR_FIRST] + [(k, 0) for k in FAR_FIRST]
    slot_at = [column.index((-k % NZ, flip)) for k, flip in column]
    others = NX * NZ - 1
    peers_y = [at(0, k, 0) for k in range(NY)]

    barrier = pltpu.get_barrier_semaphore()
    for to in peers_y[1:] + [at(k, 0, flip) for k, flip in column[:-1]]:
        pl.semaphore_signal(barrier, inc=1, device_id={"bank": to}, device_id_type=MESH)

    loads = [
        pltpu.make_async_copy(table_hbm.at[:, pl.ds(0, 128)], tab.at[0, 0], load_sem.at[0]),
        pltpu.make_async_copy(table_hbm.at[:, pl.ds(128, 128)], tab.at[1, 0], load_sem.at[6]),
        pltpu.make_async_copy(ids_hbm, idb.at[others], load_sem.at[1]),
        pltpu.make_async_copy(small_hbm, smb.at[0, others], load_sem.at[2]),
        pltpu.make_async_copy(dense_hbm, dense, load_sem.at[3]),
        pltpu.make_async_copy(small_ids_hbm, picks.at[0], load_sem.at[4]),
        pltpu.make_async_copy(scale_ids_hbm, picks.at[1], load_sem.at[5]),
    ]
    for load in loads:
        load.start()
    for load in loads:
        load.wait()
    pl.semaphore_wait(barrier, NY - 1 + others)

    half = rows // 2
    towards = ((peers_y[1], NY - 1), (peers_y[NY - 1], 1))
    def to_neighbour(up, relayed):
        to, slot = towards[up]
        piece = pl.ds((up if relayed else 1 - up) * half, half)
        remote(
            tab.at[1, 0, piece],
            tab.at[1, slot, piece],
            send_sem.at[0],
            up_sem.at[up] if relayed else y_sem.at[1],
            to,
        ).start()

    for up in range(2):
        to_neighbour(up, True)
    for k in (1, 3, 2):
        remote(tab.at[0, 0], tab.at[0, NY - k], send_sem.at[0], y_sem.at[0], peers_y[k]).start()
    for up in range(2):
        to_neighbour(up, False)
    for buf, i in ((idb, 1), (smb.at[0], 2)):
        for (k, flip), slot in zip(column[:-1], slot_at):
            remote(
                buf.at[others], buf.at[slot], send_sem.at[i], recv_sem.at[i], at(k, 0, flip)
            ).start()

    def all_of(ref, send, recv):
        return remote(ref, ref, send, recv, peers_y[1])

    for up in range(2):
        to, slot = towards[up]
        piece = pl.ds(up * half, half)
        all_of(tab.at[1, slot, piece], send_sem.at[0], up_sem.at[up]).wait_recv()
        remote(
            tab.at[1, slot, piece], tab.at[1, 2, piece], send_sem.at[0], y_sem.at[1], to
        ).start()

    ids_all = all_of(idb.at[pl.ds(0, others)], send_sem.at[1], recv_sem.at[1])
    ids_all.wait_recv()
    cols = idb[...].reshape(NX * NZ * PICKS, examples).T
    wide = [
        jnp.broadcast_to(cols[:, c : c + 1], (examples, 128)) for c in range(NX * NZ * PICKS)
    ]
    lane = lax.broadcasted_iota(jnp.int32, (examples, 128), 1)
    for ky in range(NY):
        for cut in range(0, rows, 128):
            here = lane + (peers_y[ky] * rows + cut)
            for d in range(NX * NZ):
                first = jnp.where(wide[PICKS * d] == here, 1.0, 0.0)
                count = jnp.where(wide[PICKS * d + 1] == here, first + 1.0, first)
                onehot[
                    d * examples : (d + 1) * examples, ky * rows + cut : ky * rows + cut + 128
                ] = count.astype(jnp.bfloat16)

    block = NZ * examples

    def partial(h, first):
        total = jnp.dot(
            onehot[first : first + block, :],
            tab[h].reshape(NY * rows, 128),
            preferred_element_type=jnp.float32,
        )
        return total.reshape(NZ, examples, 128)

    def swap(h, i):
        return remote(x_out.at[h, i], x_in.at[h, i], send_sem.at[3], x_sem.at[h, i], at(0, 0, 1))

    for h in range(2):
        all_of(tab.at[h, pl.ds(1, 3 - h)], send_sem.at[0], y_sem.at[h]).wait_recv()
        x_out[h] = partial(h, 0)
        for i in range(NZ - 1):
            swap(h, i).start()
        part[h] = partial(h, block)
    for h in range(2):
        swap(h, NZ - 1).start()

    sm_all = all_of(smb.at[0, pl.ds(0, others)], send_sem.at[2], recv_sem.at[2])
    sm_all.wait_recv()
    for k in (2, 1, 3):
        remote(
            smb.at[0], smb.at[NY - k], send_sem.at[4], recv_sem.at[4], peers_y[k]
        ).start()

    for h in range(2):
        for i, k in enumerate(FAR_FIRST[:-1]):
            swap(h, i).wait_recv()
            z_out[h, i] = part[h, i] + x_in[h, i]
            remote(
                z_out.at[h, i],
                z_in.at[h, FAR_FIRST.index(-k % NZ)],
                send_sem.at[5],
                recv_sem.at[5],
                at(k, 0, 0),
            ).start()

    sm_y = all_of(smb.at[pl.ds(1, NY - 1)], send_sem.at[4], recv_sem.at[4])
    sm_y.wait_recv()
    count = NY * NX * NZ * 2
    small = smb[...].reshape(count, 256)
    place = lax.broadcasted_iota(jnp.int32, (examples, count), 1)
    spot = lax.rem(place // 2, NX * NZ)
    sx = jnp.where(spot < NZ, 1 - x, x)
    sz = z
    for i, k in enumerate(FAR_FIRST):
        sz = jnp.where(lax.rem(spot, NZ) == i, lax.rem(z + k, NZ), sz)
    sy = lax.rem(place // (2 * NZ * NX) + y, NY)
    row = ((sz * NY + sy) * NX + sx) * 2 + lax.rem(place, 2)
    pick_cols = picks[...].reshape(2, examples).T
    found = [
        jnp.dot(
            jnp.where(pick_cols[:, i : i + 1] == row, 1.0, 0.0).astype(jnp.bfloat16),
            small,
            preferred_element_type=jnp.float32,
        )
        for i in range(2)
    ]
    scaled = dense[...] * found[1]

    for h in range(2):
        swap(h, NZ - 1).wait_recv()

    z_all = all_of(z_in, send_sem.at[5], recv_sem.at[5])
    z_all.wait_recv()
    totals = []
    for h in range(2):
        pooled = part[h, NZ - 1] + x_in[h, NZ - 1]
        for i in range(NZ - 1):
            pooled += z_in[h, i]
        cut = slice(h * 128, (h + 1) * 128)
        totals.append(scaled[:, cut] + pooled * PICKS ** (-0.5) * found[0][:, cut])
    square = totals[0] * totals[0] + totals[1] * totals[1]
    power = jnp.sum(square, axis=-1, keepdims=True) / 256.0
    inverse = lax.rsqrt(power + 1e-06)
    for h in range(2):
        out_ref[:, h * 128 : (h + 1) * 128] = totals[h] * inverse

    all_of(tab.at[:, pl.ds(1, 3)], send_sem.at[0], y_sem.at[0]).wait_send()
    ids_all.wait_send()
    sm_all.wait_send()
    all_of(x_out, send_sem.at[3], recv_sem.at[3]).wait_send()
    sm_y.wait_send()
    all_of(z_out, send_sem.at[5], recv_sem.at[5]).wait_send()


def shards(item_ids, large_table, dense_part, small_ids, small_table, scale_ids):
    examples, features = dense_part.shape
    rows = large_table.shape[0]
    any_space = pl.BlockSpec(memory_space=pl.ANY)
    dma = pltpu.SemaphoreType.DMA
    block = (examples, 128)
    return pl.pallas_call(
        kernel,
        out_shape=pltpu.VMEM((examples, features), jnp.float32),
        in_specs=[any_space] * 6,
        out_specs=pl.BlockSpec(memory_space=pltpu.VMEM),
        scratch_shapes=[
            pltpu.VMEM((2, NY, rows, 128), jnp.bfloat16),
            pltpu.VMEM((NX * NZ, PICKS, examples), jnp.int32),
            pltpu.VMEM((NY, NX * NZ, 2, features), jnp.bfloat16),
            pltpu.VMEM((examples, features), jnp.float32),
            pltpu.VMEM((2, 1, examples), jnp.int32),
            pltpu.VMEM((NX * NZ * examples, NY * rows), jnp.bfloat16),
            pltpu.VMEM((2, NZ, *block), jnp.float32),
            pltpu.VMEM((2, NZ, *block), jnp.float32),
            pltpu.VMEM((2, NZ, *block), jnp.float32),
            pltpu.VMEM((2, NZ - 1, *block), jnp.float32),
            pltpu.VMEM((2, NZ - 1, *block), jnp.float32),
            dma((7,)),
            dma((6,)),
            dma((6,)),
            dma((2, NZ)),
            dma((2,)),
            dma((2,)),
        ],
        compiler_params=pltpu.CompilerParams(collective_id=0, has_side_effects=True),
    )(
        item_ids.T,
        large_table,
        dense_part,
        small_ids.reshape(1, examples),
        scale_ids.reshape(1, examples),
        small_table,
    )


def solution(mesh):
    return jax.shard_map(
        shards,
        mesh=mesh,
        in_specs=(
            P(("ens", "bank"), None),
            P(("ens", "bank"), None),
            P(("ens", "bank"), None),
            P(("ens", "bank")),
            P(("ens", "bank"), None),
            P(("ens", "bank")),
        ),
        out_specs=P(("ens", "bank"), None),
        check_vma=False,
    )
```

```python
import functools

import jax
import jax.numpy as jnp
from jax import lax
from jax.experimental import pallas as pl
from jax.experimental.pallas import tpu as pltpu
from jax.sharding import PartitionSpec as P

PICKS = 2
NZ, NY, NX = 8, 4, 2
NEAR, COLUMN = 4, 16
OTHERS = COLUMN - 1
FAR_0 = (4, 5, 7, 6, 2, 3, 1, 0)
FAR_1 = (2, 3, 1, 0)
COLUMN_0 = [(f, k) for group in (FAR_0[:2], FAR_0[2:4], FAR_0[4:]) for f in (1, 0) for k in group]
COLUMN_1 = [
    pair
    for group in (FAR_1[:1], FAR_1[1:2], FAR_1[2:])
    for pair in [(f, k) for k in group for f in FAR_1[:-1]] + [(0, k) for k in group]
]
GROUPS = ((0, 4), (4, 4), (8, 8))
NEAREST = 2
MESH = pl.DeviceIdType.MESH


def kernel(
    ids_hbm,
    table_hbm,
    dense_hbm,
    small_ids_hbm,
    scale_ids_hbm,
    small_hbm,
    out_ref,
    tab,
    idb,
    smb,
    dense,
    picks,
    onehot,
    part,
    x_out,
    x_in,
    z_out,
    z_in,
    load_sem,
    send_sem,
    recv_sem,
    x_sem,
    y_sem,
    ids_sem,
):
    bank = lax.axis_index("bank")
    x = lax.rem(bank, NX)
    y = lax.rem(bank // NX, NY)
    z = bank // (NX * NY)
    second = lax.rem(lax.axis_index("ens"), 2) == 1

    def plan(first_core, second_core):
        return jnp.where(second, second_core, first_core)

    def flip(value, bit):
        return 1 - value if bit else value

    def change(value, bits):
        return sum(flip(lax.rem(value // b, 2), bits // b % 2) * b for b in (1, 2, 4))

    near = [
        plan(
            change(y, k) * NX,
            change(lax.rem(z, 2), k // 2) * (NY * NX) + change(x, k % 2 ^ k // 2),
        )
        for k in range(NEAR)
    ]

    def column_0(f, k):
        return change(x, f) + change(z, k) * (NY * NX)

    def column_1(f, k):
        return change(y, f) * NX + change(z // 2, k) * (2 * NY * NX)

    column = [plan(column_0(*COLUMN_0[i]), column_1(*COLUMN_1[i])) for i in range(COLUMN)]

    def remote(src, dst, send, recv, to):
        return pltpu.make_async_remote_copy(
            src_ref=src,
            dst_ref=dst,
            send_sem=send,
            recv_sem=recv,
            device_id={"bank": to},
            device_id_type=MESH,
        )

    rows = table_hbm.shape[0]
    examples = dense_hbm.shape[0]
    sharers = [near[k] + column[OTHERS] for k in range(NEAR)]
    askers = [near[0] + column[i] for i in range(OTHERS)]

    barrier = pltpu.get_barrier_semaphore()
    for to in sharers[1:] + askers:
        pl.semaphore_signal(barrier, inc=1, device_id={"bank": to}, device_id_type=MESH)

    loads = [
        pltpu.make_async_copy(table_hbm.at[:, pl.ds(0, 128)], tab.at[0, 0], load_sem.at[0]),
        pltpu.make_async_copy(table_hbm.at[:, pl.ds(128, 128)], tab.at[1, 0], load_sem.at[0]),
        pltpu.make_async_copy(ids_hbm, idb.at[OTHERS], load_sem.at[1]),
        pltpu.make_async_copy(small_hbm, smb.at[0, OTHERS], load_sem.at[2]),
        pltpu.make_async_copy(dense_hbm, dense, load_sem.at[3]),
        pltpu.make_async_copy(small_ids_hbm, picks.at[0], load_sem.at[4]),
        pltpu.make_async_copy(scale_ids_hbm, picks.at[1], load_sem.at[4]),
    ]
    for load in loads:
        load.start()
    for buf, i in (
        (tab.at[:, 0], 0), (idb.at[OTHERS], 1), (smb.at[0, OTHERS], 2), (dense, 3), (picks, 4)
    ):
        pltpu.make_async_copy(buf, buf, load_sem.at[i]).wait()
    pl.semaphore_wait(barrier, NEAR - 1 + OTHERS)

    for i in range(OTHERS):
        remote(
            idb.at[OTHERS],
            idb.at[i],
            send_sem.at[1],
            ids_sem.at[min(i // 4, NEAREST)],
            askers[i],
        ).start()
    for i in range(OTHERS):
        remote(
            smb.at[0, OTHERS],
            smb.at[0, i],
            send_sem.at[2],
            recv_sem.at[2],
            askers[i],
        ).start()
    for h in range(2):
        for k in (2, 1, 3):
            remote(
                tab.at[h, 0], tab.at[h, k], send_sem.at[0], y_sem.at[h], sharers[k]
            ).start()
    def all_of(ref, send, recv):
        return remote(ref, ref, send, recv, sharers[1])

    lane = lax.broadcasted_iota(jnp.int32, (examples, 128), 1)

    def mark_rows(group):
        first, blocks = GROUPS[group]
        arrived = idb.at[pl.ds(first, blocks - (group == NEAREST))]
        all_of(arrived, send_sem.at[1], ids_sem.at[group]).wait_recv()
        cols = idb[first : first + blocks].reshape(blocks * PICKS, examples).T
        wide = [
            jnp.broadcast_to(cols[:, c : c + 1], (examples, 128)) for c in range(blocks * PICKS)
        ]
        for k in range(NEAR):
            for cut in range(0, rows, 128):
                here = lane + (sharers[k] * rows + cut)
                for d in range(blocks):
                    once = jnp.where(wide[PICKS * d] == here, 1.0, 0.0)
                    count = jnp.where(wide[PICKS * d + 1] == here, once + 1.0, once)
                    onehot[
                        (first + d) * examples : (first + d + 1) * examples,
                        k * rows + cut : k * rows + cut + 128,
                    ] = count.astype(jnp.bfloat16)

    mark_rows(NEAREST)

    def partial(h, first, blocks):
        total = jnp.dot(
            onehot[first * examples : (first + blocks) * examples, :],
            tab[h].reshape(NEAR * rows, 128),
            preferred_element_type=jnp.float32,
        )
        return total.reshape(blocks, examples, 128)

    def wait_rows(h):
        all_of(tab.at[h, pl.ds(1, NEAR - 1)], send_sem.at[0], y_sem.at[h]).wait_recv()

    def by_core(steps):
        pl.when(jnp.logical_not(second))(functools.partial(steps, True))
        pl.when(second)(functools.partial(steps, False))

    def planes(first_core):
        return (len(FAR_0), 1) if first_core else (len(FAR_1), len(FAR_1) - 1)

    def first_peer(first_core, f):
        if first_core:
            return near[0] + column_0(1, 0)
        return near[0] + column_1(f, 0)

    def first_step(first_core):
        count, each = planes(first_core)
        width = count * each

        def send(h, i):
            k, j = i // each, i % each
            f = 1 if first_core else FAR_1[j]
            remote(
                x_out.at[h, i],
                x_in.at[h, i],
                send_sem.at[3],
                x_sem.at[h, k] if k < count - 1 else recv_sem.at[3],
                first_peer(first_core, f),
            ).start()

        def sums(h, group):
            first, blocks = GROUPS[group]
            k, planes_here = first * count // COLUMN, blocks * count // COLUMN
            outs = planes_here * each
            x_out[h, k * each : k * each + outs] = partial(h, first, outs)
            for i in range(k * each, min(k * each + outs, width - each)):
                send(h, i)

        def keep(h, group):
            first, blocks = GROUPS[group]
            k, planes_here = first * count // COLUMN, blocks * count // COLUMN
            part[h, k : k + planes_here] = partial(h, first + planes_here * each, planes_here)

        wait_rows(0)
        sums(0, NEAREST)
        for group in (1, 0):
            mark_rows(group)
            sums(0, group)
        wait_rows(1)
        for group in (2, 1, 0):
            sums(1, group)
        for h in range(2):
            for i in range(width - each, width):
                send(h, i)
        for group in (NEAREST, 1, 0):
            for h in range(2):
                keep(h, group)

    by_core(first_step)

    sm_all = all_of(smb.at[0, pl.ds(0, OTHERS)], send_sem.at[2], recv_sem.at[2])
    sm_all.wait_recv()
    for k in (2, 1, 3):
        remote(
            smb.at[0], smb.at[k], send_sem.at[4], recv_sem.at[4], sharers[k]
        ).start()

    def second_step(first_core):
        count, each = planes(first_core)
        half, quarter = count // 2, count // 4
        spans = ((0, quarter), (quarter, half), (half, count - 1))
        for h, group in [(0, 2), (0, 1), (0, 0)] + [(1, g) for g in (2, 1, 0)]:
            for k in range(*spans[group]):
                arrived = x_in.at[h, pl.ds(k * each, each)]
                all_of(arrived, send_sem.at[3], x_sem.at[h, k]).wait_recv()
                total = part[h, k]
                for j in range(each):
                    total += x_in[h, k * each + j]
                z_out[h, k] = total
                to = column_0(0, FAR_0[k]) if first_core else column_1(0, FAR_1[k])
                remote(
                    z_out.at[h, k],
                    z_in.at[h, k],
                    send_sem.at[5],
                    recv_sem.at[5],
                    near[0] + to,
                ).start()

    by_core(second_step)

    sm_y = all_of(smb.at[pl.ds(1, NEAR - 1)], send_sem.at[4], recv_sem.at[4])
    sm_y.wait_recv()
    count = NEAR * COLUMN * 2
    small = smb[...].reshape(count, 256)
    place = lax.broadcasted_iota(jnp.int32, (examples, count), 1)

    def chosen(values, index):
        result = values[0]
        for i in range(1, len(values)):
            result = jnp.where(index == i, values[i], result)
        return result

    holder = chosen(near, place // (2 * COLUMN)) + chosen(column, lax.rem(place // 2, COLUMN))
    row = holder * 2 + lax.rem(place, 2)
    pick_cols = picks[...].reshape(2, examples).T
    found = [
        jnp.dot(
            jnp.where(pick_cols[:, i : i + 1] == row, 1.0, 0.0).astype(jnp.bfloat16),
            small,
            preferred_element_type=jnp.float32,
        )
        for i in range(2)
    ]
    scaled = dense[...] * found[1]

    def collect(first_core):
        count, each = planes(first_core)
        own = pl.ds((count - 1) * each, each)
        all_of(x_in.at[:, own], send_sem.at[3], recv_sem.at[3]).wait_recv()
        all_of(z_in.at[:, pl.ds(0, count - 1)], send_sem.at[5], recv_sem.at[5]).wait_recv()
        for h in range(2):
            total = part[h, count - 1]
            for j in range(each):
                total += x_in[h, (count - 1) * each + j]
            for k in range(count - 1):
                total += z_in[h, k]
            part[h, 0] = total
        all_of(x_out.at[:, pl.ds(0, count * each)], send_sem.at[3], recv_sem.at[3]).wait_send()
        all_of(z_out.at[:, pl.ds(0, count - 1)], send_sem.at[5], recv_sem.at[5]).wait_send()

    by_core(collect)
    totals = []
    for h in range(2):
        pooled = part[h, 0]
        cut = slice(h * 128, (h + 1) * 128)
        totals.append(scaled[:, cut] + pooled * PICKS ** (-0.5) * found[0][:, cut])
    square = totals[0] * totals[0] + totals[1] * totals[1]
    power = jnp.sum(square, axis=-1, keepdims=True) / 256.0
    inverse = lax.rsqrt(power + 1e-06)
    for h in range(2):
        out_ref[:, h * 128 : (h + 1) * 128] = totals[h] * inverse

    all_of(tab.at[:, pl.ds(1, 3)], send_sem.at[0], y_sem.at[0]).wait_send()
    all_of(idb.at[pl.ds(0, OTHERS)], send_sem.at[1], recv_sem.at[1]).wait_send()
    sm_all.wait_send()
    sm_y.wait_send()


def shards(item_ids, large_table, dense_part, small_ids, small_table, scale_ids):
    examples, features = dense_part.shape
    rows = large_table.shape[0]
    any_space = pl.BlockSpec(memory_space=pl.ANY)
    dma = pltpu.SemaphoreType.DMA
    block = (examples, 128)
    return pl.pallas_call(
        kernel,
        out_shape=pltpu.VMEM((examples, features), jnp.float32),
        in_specs=[any_space] * 6,
        out_specs=pl.BlockSpec(memory_space=pltpu.VMEM),
        scratch_shapes=[
            pltpu.VMEM((2, NEAR, rows, 128), jnp.bfloat16),
            pltpu.VMEM((COLUMN, PICKS, examples), jnp.int32),
            pltpu.VMEM((NEAR, COLUMN, 2, features), jnp.bfloat16),
            pltpu.VMEM((examples, features), jnp.float32),
            pltpu.VMEM((2, 1, examples), jnp.int32),
            pltpu.VMEM((COLUMN * examples, NEAR * rows), jnp.bfloat16),
            pltpu.VMEM((2, 8, *block), jnp.float32),
            pltpu.VMEM((2, 12, *block), jnp.float32),
            pltpu.VMEM((2, 12, *block), jnp.float32),
            pltpu.VMEM((2, 7, *block), jnp.float32),
            pltpu.VMEM((2, 7, *block), jnp.float32),
            dma((5,)),
            dma((6,)),
            dma((6,)),
            dma((2, 7)),
            dma((2,)),
            dma((len(GROUPS),)),
        ],
        compiler_params=pltpu.CompilerParams(collective_id=0, has_side_effects=True),
    )(
        item_ids.T,
        large_table,
        dense_part,
        small_ids.reshape(1, examples),
        scale_ids.reshape(1, examples),
        small_table,
    )


def solution(mesh):
    return jax.shard_map(
        shards,
        mesh=mesh,
        in_specs=(
            P(("ens", "bank"), None),
            P(("ens", "bank"), None),
            P(("ens", "bank"), None),
            P(("ens", "bank")),
            P(("ens", "bank"), None),
            P(("ens", "bank")),
        ),
        out_specs=P(("ens", "bank"), None),
        check_vma=False,
    )
```

```python
import functools

import jax
import jax.numpy as jnp
from jax import lax
from jax.experimental import pallas as pl
from jax.experimental.pallas import tpu as pltpu
from jax.sharding import PartitionSpec as P

PICKS = 2
NZ, NY, NX = 8, 4, 2
NEAR, COLUMN = 4, 16
OTHERS = COLUMN - 1
FAR_0 = (4, 5, 7, 6, 2, 3, 1, 0)
FAR_1 = (2, 3, 1, 0)
COLUMN_0 = [(f, k) for group in (FAR_0[:2], FAR_0[2:4], FAR_0[4:]) for f in (1, 0) for k in group]
COLUMN_1 = [
    pair
    for group in (FAR_1[:1], FAR_1[1:2], FAR_1[2:])
    for pair in [(f, k) for k in group for f in FAR_1[:-1]] + [(0, k) for k in group]
]
GROUPS = ((0, 4), (4, 4), (8, 8))
NEAREST = 2
MESH = pl.DeviceIdType.MESH


def kernel(
    ids_hbm,
    table_hbm,
    dense_hbm,
    small_ids_hbm,
    scale_ids_hbm,
    small_hbm,
    out_ref,
    tab,
    idb,
    smb,
    dense,
    picks,
    onehot,
    part,
    x_out,
    x_in,
    z_out,
    z_in,
    load_sem,
    send_sem,
    recv_sem,
    x_sem,
    y_sem,
    ids_sem,
):
    bank = lax.axis_index("bank")
    x = lax.rem(bank, NX)
    y = lax.rem(bank // NX, NY)
    z = bank // (NX * NY)
    second = lax.rem(lax.axis_index("ens"), 2) == 1

    def plan(first_core, second_core):
        return jnp.where(second, second_core, first_core)

    def flip(value, bit):
        return 1 - value if bit else value

    def change(value, bits):
        return sum(flip(lax.rem(value // b, 2), bits // b % 2) * b for b in (1, 2, 4))

    near = [
        plan(
            change(y, k) * NX,
            change(lax.rem(z, 2), k // 2) * (NY * NX) + change(x, k % 2 ^ k // 2),
        )
        for k in range(NEAR)
    ]

    def column_0(f, k):
        return change(x, f) + change(z, k) * (NY * NX)

    def column_1(f, k):
        return change(y, f) * NX + change(z // 2, k) * (2 * NY * NX)

    column = [plan(column_0(*COLUMN_0[i]), column_1(*COLUMN_1[i])) for i in range(COLUMN)]

    def remote(src, dst, send, recv, to):
        return pltpu.make_async_remote_copy(
            src_ref=src,
            dst_ref=dst,
            send_sem=send,
            recv_sem=recv,
            device_id={"bank": to},
            device_id_type=MESH,
        )

    rows = table_hbm.shape[0]
    examples = dense_hbm.shape[0]
    sharers = [near[k] + column[OTHERS] for k in range(NEAR)]
    askers = [near[0] + column[i] for i in range(OTHERS)]

    barrier = pltpu.get_barrier_semaphore()
    for to in sharers[1:] + askers:
        pl.semaphore_signal(barrier, inc=1, device_id={"bank": to}, device_id_type=MESH)

    loads = [
        pltpu.make_async_copy(table_hbm.at[:, pl.ds(0, 128)], tab.at[0, 0], load_sem.at[0]),
        pltpu.make_async_copy(table_hbm.at[:, pl.ds(128, 128)], tab.at[1, 0], load_sem.at[0]),
        pltpu.make_async_copy(ids_hbm, idb.at[OTHERS], load_sem.at[1]),
        pltpu.make_async_copy(small_hbm, smb.at[0, OTHERS], load_sem.at[2]),
        pltpu.make_async_copy(dense_hbm, dense, load_sem.at[3]),
        pltpu.make_async_copy(small_ids_hbm, picks.at[0], load_sem.at[4]),
        pltpu.make_async_copy(scale_ids_hbm, picks.at[1], load_sem.at[4]),
    ]
    for load in loads:
        load.start()
    for buf, i in (
        (tab.at[:, 0], 0), (idb.at[OTHERS], 1), (smb.at[0, OTHERS], 2), (dense, 3), (picks, 4)
    ):
        pltpu.make_async_copy(buf, buf, load_sem.at[i]).wait()
    pl.semaphore_wait(barrier, NEAR - 1 + OTHERS)

    for i in range(OTHERS):
        remote(
            idb.at[OTHERS],
            idb.at[i],
            send_sem.at[1],
            ids_sem.at[min(i // 4, NEAREST)],
            askers[i],
        ).start()
    for i in range(OTHERS):
        remote(
            smb.at[0, OTHERS],
            smb.at[0, i],
            send_sem.at[2],
            recv_sem.at[2],
            askers[i],
        ).start()
    for h in range(2):
        for k in (2, 1, 3):
            remote(
                tab.at[h, 0], tab.at[h, k], send_sem.at[0], y_sem.at[h], sharers[k]
            ).start()
    def all_of(ref, send, recv):
        return remote(ref, ref, send, recv, sharers[1])

    lane = lax.broadcasted_iota(jnp.int32, (examples, 128), 1)

    def mark_rows(group):
        first, blocks = GROUPS[group]
        arrived = idb.at[pl.ds(first, blocks - (group == NEAREST))]
        all_of(arrived, send_sem.at[1], ids_sem.at[group]).wait_recv()
        cols = idb[first : first + blocks].reshape(blocks * PICKS, examples).T
        wide = [
            jnp.broadcast_to(cols[:, c : c + 1], (examples, 128)) for c in range(blocks * PICKS)
        ]
        for k in range(NEAR):
            for cut in range(0, rows, 128):
                here = lane + (sharers[k] * rows + cut)
                for d in range(blocks):
                    once = jnp.where(wide[PICKS * d] == here, 1.0, 0.0)
                    count = jnp.where(wide[PICKS * d + 1] == here, once + 1.0, once)
                    onehot[
                        (first + d) * examples : (first + d + 1) * examples,
                        k * rows + cut : k * rows + cut + 128,
                    ] = count.astype(jnp.bfloat16)

    mark_rows(NEAREST)

    def partial(h, first, blocks):
        total = jnp.dot(
            onehot[first * examples : (first + blocks) * examples, :],
            tab[h].reshape(NEAR * rows, 128),
            preferred_element_type=jnp.float32,
        )
        return total.reshape(blocks, examples, 128)

    def wait_rows(h):
        all_of(tab.at[h, pl.ds(1, NEAR - 1)], send_sem.at[0], y_sem.at[h]).wait_recv()

    def by_core(steps):
        pl.when(jnp.logical_not(second))(functools.partial(steps, True))
        pl.when(second)(functools.partial(steps, False))

    def planes(first_core):
        return (len(FAR_0), 1) if first_core else (len(FAR_1), len(FAR_1) - 1)

    def in_order(first_core, steps):
        if not first_core:
            return steps((2, 1, 0))
        late = z >= NZ // 2
        pl.when(late)(functools.partial(steps, (0, 1, 2)))
        pl.when(jnp.logical_not(late))(functools.partial(steps, (2, 1, 0)))

    def first_peer(first_core, f):
        if first_core:
            return near[0] + column_0(1, 0)
        return near[0] + column_1(f, 0)

    def first_step(first_core):
        count, each = planes(first_core)
        width = count * each

        def send(h, i):
            k, j = i // each, i % each
            f = 1 if first_core else FAR_1[j]
            remote(
                x_out.at[h, i],
                x_in.at[h, i],
                send_sem.at[3],
                x_sem.at[h, k] if k < count - 1 else recv_sem.at[3],
                first_peer(first_core, f),
            ).start()

        def sums(h, group):
            first, blocks = GROUPS[group]
            k, planes_here = first * count // COLUMN, blocks * count // COLUMN
            outs = planes_here * each
            x_out[h, k * each : k * each + outs] = partial(h, first, outs)
            for i in range(k * each, min(k * each + outs, width - each)):
                send(h, i)

        def keep(h, group):
            first, blocks = GROUPS[group]
            k, planes_here = first * count // COLUMN, blocks * count // COLUMN
            part[h, k : k + planes_here] = partial(h, first + planes_here * each, planes_here)

        wait_rows(0)
        sums(0, NEAREST)
        for group in (1, 0):
            mark_rows(group)
            sums(0, group)
        wait_rows(1)

        def second_half(order):
            for group in order:
                sums(1, group)

        in_order(first_core, second_half)
        for h in range(2):
            for i in range(width - each, width):
                send(h, i)
        for group in (NEAREST, 1, 0):
            for h in range(2):
                keep(h, group)

    by_core(first_step)

    sm_all = all_of(smb.at[0, pl.ds(0, OTHERS)], send_sem.at[2], recv_sem.at[2])
    sm_all.wait_recv()
    for k in (2, 1, 3):
        remote(
            smb.at[0], smb.at[k], send_sem.at[4], recv_sem.at[4], sharers[k]
        ).start()

    def second_step(first_core):
        count, each = planes(first_core)
        half, quarter = count // 2, count // 4
        spans = ((0, quarter), (quarter, half), (half, count - 1))

        def pass_on(h, order):
            for k in [k for group in order for k in range(*spans[group])]:
                arrived = x_in.at[h, pl.ds(k * each, each)]
                all_of(arrived, send_sem.at[3], x_sem.at[h, k]).wait_recv()
                total = part[h, k]
                for j in range(each):
                    total += x_in[h, k * each + j]
                z_out[h, k] = total
                to = column_0(0, FAR_0[k]) if first_core else column_1(0, FAR_1[k])
                remote(
                    z_out.at[h, k],
                    z_in.at[h, k],
                    send_sem.at[5],
                    recv_sem.at[5],
                    near[0] + to,
                ).start()

        pass_on(0, (2, 1, 0))
        in_order(first_core, functools.partial(pass_on, 1))

    by_core(second_step)

    sm_y = all_of(smb.at[pl.ds(1, NEAR - 1)], send_sem.at[4], recv_sem.at[4])
    sm_y.wait_recv()
    count = NEAR * COLUMN * 2
    small = smb[...].reshape(count, 256)
    place = lax.broadcasted_iota(jnp.int32, (examples, count), 1)

    def chosen(values, index):
        result = values[0]
        for i in range(1, len(values)):
            result = jnp.where(index == i, values[i], result)
        return result

    holder = chosen(near, place // (2 * COLUMN)) + chosen(column, lax.rem(place // 2, COLUMN))
    row = holder * 2 + lax.rem(place, 2)
    pick_cols = picks[...].reshape(2, examples).T
    found = [
        jnp.dot(
            jnp.where(pick_cols[:, i : i + 1] == row, 1.0, 0.0).astype(jnp.bfloat16),
            small,
            preferred_element_type=jnp.float32,
        )
        for i in range(2)
    ]
    scaled = dense[...] * found[1]

    def collect(first_core):
        count, each = planes(first_core)
        own = pl.ds((count - 1) * each, each)
        all_of(x_in.at[:, own], send_sem.at[3], recv_sem.at[3]).wait_recv()
        all_of(z_in.at[:, pl.ds(0, count - 1)], send_sem.at[5], recv_sem.at[5]).wait_recv()
        for h in range(2):
            total = part[h, count - 1]
            for j in range(each):
                total += x_in[h, (count - 1) * each + j]
            for k in range(count - 1):
                total += z_in[h, k]
            part[h, 0] = total
        all_of(x_out.at[:, pl.ds(0, count * each)], send_sem.at[3], recv_sem.at[3]).wait_send()
        all_of(z_out.at[:, pl.ds(0, count - 1)], send_sem.at[5], recv_sem.at[5]).wait_send()

    by_core(collect)
    totals = []
    for h in range(2):
        pooled = part[h, 0]
        cut = slice(h * 128, (h + 1) * 128)
        totals.append(scaled[:, cut] + pooled * PICKS ** (-0.5) * found[0][:, cut])
    square = totals[0] * totals[0] + totals[1] * totals[1]
    power = jnp.sum(square, axis=-1, keepdims=True) / 256.0
    inverse = lax.rsqrt(power + 1e-06)
    for h in range(2):
        out_ref[:, h * 128 : (h + 1) * 128] = totals[h] * inverse

    all_of(tab.at[:, pl.ds(1, 3)], send_sem.at[0], y_sem.at[0]).wait_send()
    all_of(idb.at[pl.ds(0, OTHERS)], send_sem.at[1], recv_sem.at[1]).wait_send()
    sm_all.wait_send()
    sm_y.wait_send()


def shards(item_ids, large_table, dense_part, small_ids, small_table, scale_ids):
    examples, features = dense_part.shape
    rows = large_table.shape[0]
    any_space = pl.BlockSpec(memory_space=pl.ANY)
    dma = pltpu.SemaphoreType.DMA
    block = (examples, 128)
    return pl.pallas_call(
        kernel,
        out_shape=pltpu.VMEM((examples, features), jnp.float32),
        in_specs=[any_space] * 6,
        out_specs=pl.BlockSpec(memory_space=pltpu.VMEM),
        scratch_shapes=[
            pltpu.VMEM((2, NEAR, rows, 128), jnp.bfloat16),
            pltpu.VMEM((COLUMN, PICKS, examples), jnp.int32),
            pltpu.VMEM((NEAR, COLUMN, 2, features), jnp.bfloat16),
            pltpu.VMEM((examples, features), jnp.float32),
            pltpu.VMEM((2, 1, examples), jnp.int32),
            pltpu.VMEM((COLUMN * examples, NEAR * rows), jnp.bfloat16),
            pltpu.VMEM((2, 8, *block), jnp.float32),
            pltpu.VMEM((2, 12, *block), jnp.float32),
            pltpu.VMEM((2, 12, *block), jnp.float32),
            pltpu.VMEM((2, 7, *block), jnp.float32),
            pltpu.VMEM((2, 7, *block), jnp.float32),
            dma((5,)),
            dma((6,)),
            dma((6,)),
            dma((2, 7)),
            dma((2,)),
            dma((len(GROUPS),)),
        ],
        compiler_params=pltpu.CompilerParams(collective_id=0, has_side_effects=True),
    )(
        item_ids.T,
        large_table,
        dense_part,
        small_ids.reshape(1, examples),
        scale_ids.reshape(1, examples),
        small_table,
    )


def solution(mesh):
    return jax.shard_map(
        shards,
        mesh=mesh,
        in_specs=(
            P(("ens", "bank"), None),
            P(("ens", "bank"), None),
            P(("ens", "bank"), None),
            P(("ens", "bank")),
            P(("ens", "bank"), None),
            P(("ens", "bank")),
        ),
        out_specs=P(("ens", "bank"), None),
        check_vma=False,
    )
```

```python
import functools

import jax
import jax.numpy as jnp
from jax import lax
from jax.experimental import pallas as pl
from jax.experimental.pallas import tpu as pltpu
from jax.sharding import PartitionSpec as P

PICKS = 2
NZ, NY, NX = 8, 4, 2
NEAR, COLUMN = 4, 16
OTHERS = COLUMN - 1
FAR_0 = (4, 5, 7, 6, 3, 2, 1, 0)
FAR_1 = (2, 3, 1, 0)
COLUMN_0 = [(f, k) for group in (FAR_0[:2], FAR_0[2:4], FAR_0[4:]) for f in (1, 0) for k in group]
COLUMN_1 = [
    pair
    for group in (FAR_1[:1], FAR_1[1:2], FAR_1[2:])
    for pair in [(f, k) for k in group for f in FAR_1[:-1]] + [(0, k) for k in group]
]
GROUPS = ((0, 4), (4, 4), (8, 8))
NEAREST = 2
MESH = pl.DeviceIdType.MESH


def kernel(
    ids_hbm,
    table_hbm,
    dense_hbm,
    small_ids_hbm,
    scale_ids_hbm,
    small_hbm,
    out_ref,
    tab,
    idb,
    smb,
    dense,
    picks,
    onehot,
    part,
    x_out,
    x_in,
    z_out,
    z_in,
    here_sem,
    recv_sem,
    x_sem,
    y_sem,
    ids_sem,
):
    bank = lax.axis_index("bank")
    x = lax.rem(bank, NX)
    y = lax.rem(bank // NX, NY)
    z = bank // (NX * NY)
    second = lax.rem(lax.axis_index("ens"), 2) == 1

    def plan(first_core, second_core):
        return jnp.where(second, second_core, first_core)

    def flip(value, bit):
        return 1 - value if bit else value

    def change(value, bits):
        return sum(flip(lax.rem(value // b, 2), bits // b % 2) * b for b in (1, 2, 4))

    near = [
        plan(
            change(y, k) * NX,
            change(lax.rem(z, 2), k // 2) * (NY * NX) + change(x, k % 2 ^ k // 2),
        )
        for k in range(NEAR)
    ]

    def column_0(f, k):
        return change(x, f) + change(z, k) * (NY * NX)

    def column_1(f, k):
        return change(y, f) * NX + change(z // 2, k) * (2 * NY * NX)

    column = [plan(column_0(*COLUMN_0[i]), column_1(*COLUMN_1[i])) for i in range(COLUMN)]

    def remote(src, dst, send, recv, to):
        return pltpu.make_async_remote_copy(
            src_ref=src,
            dst_ref=dst,
            send_sem=send,
            recv_sem=recv,
            device_id={"bank": to},
            device_id_type=MESH,
        )

    rows = table_hbm.shape[0]
    examples = dense_hbm.shape[0]
    sharers = [near[k] + column[OTHERS] for k in range(NEAR)]
    askers = [near[0] + column[i] for i in range(OTHERS)]

    barrier = pltpu.get_barrier_semaphore()
    for to in sharers[1:] + askers:
        pl.semaphore_signal(barrier, inc=1, device_id={"bank": to}, device_id_type=MESH)

    loads = [
        pltpu.make_async_copy(table_hbm.at[:, pl.ds(0, 128)], tab.at[0, 0], here_sem.at[0]),
        pltpu.make_async_copy(table_hbm.at[:, pl.ds(128, 128)], tab.at[1, 0], here_sem.at[0]),
        pltpu.make_async_copy(ids_hbm, idb.at[OTHERS], here_sem.at[1]),
        pltpu.make_async_copy(small_hbm, smb.at[0, OTHERS], here_sem.at[2]),
        pltpu.make_async_copy(dense_hbm, dense, here_sem.at[3]),
        pltpu.make_async_copy(small_ids_hbm, picks.at[0], here_sem.at[4]),
        pltpu.make_async_copy(scale_ids_hbm, picks.at[1], here_sem.at[4]),
    ]
    for load in loads:
        load.start()
    for buf, i in (
        (tab.at[:, 0], 0), (idb.at[OTHERS], 1), (smb.at[0, OTHERS], 2), (dense, 3), (picks, 4)
    ):
        pltpu.make_async_copy(buf, buf, here_sem.at[i]).wait()
    pl.semaphore_wait(barrier, NEAR - 1 + OTHERS)

    for i in range(OTHERS):
        remote(
            idb.at[OTHERS],
            idb.at[i],
            here_sem.at[1],
            ids_sem.at[min(i // 4, NEAREST)],
            askers[i],
        ).start()
    for i in range(OTHERS):
        remote(
            smb.at[0, OTHERS],
            smb.at[0, i],
            here_sem.at[2],
            recv_sem.at[2],
            askers[i],
        ).start()
    for h in range(2):
        for k in (2, 1, 3):
            remote(
                tab.at[h, 0], tab.at[h, k], here_sem.at[0], y_sem.at[h], sharers[k]
            ).start()
    def all_of(ref, send, recv):
        return remote(ref, ref, send, recv, sharers[1])

    lane = lax.broadcasted_iota(jnp.int32, (examples, 128), 1)

    def mark_rows(group):
        first, blocks = GROUPS[group]
        arrived = idb.at[pl.ds(first, blocks - (group == NEAREST))]
        all_of(arrived, here_sem.at[1], ids_sem.at[group]).wait_recv()
        cols = idb[first : first + blocks].reshape(blocks * PICKS, examples).T
        wide = [
            jnp.broadcast_to(cols[:, c : c + 1], (examples, 128)) for c in range(blocks * PICKS)
        ]
        for k in range(NEAR):
            for cut in range(0, rows, 128):
                here = lane + (sharers[k] * rows + cut)
                for d in range(blocks):
                    once = jnp.where(wide[PICKS * d] == here, 1.0, 0.0)
                    count = jnp.where(wide[PICKS * d + 1] == here, once + 1.0, once)
                    onehot[
                        (first + d) * examples : (first + d + 1) * examples,
                        k * rows + cut : k * rows + cut + 128,
                    ] = count.astype(jnp.bfloat16)

    mark_rows(NEAREST)

    def partial(h, first, blocks):
        total = jnp.dot(
            onehot[first * examples : (first + blocks) * examples, :],
            tab[h].reshape(NEAR * rows, 128),
            preferred_element_type=jnp.float32,
        )
        return total.reshape(blocks, examples, 128)

    def wait_rows(h):
        all_of(tab.at[h, pl.ds(1, NEAR - 1)], here_sem.at[0], y_sem.at[h]).wait_recv()

    def by_core(steps):
        pl.when(jnp.logical_not(second))(functools.partial(steps, True))
        pl.when(second)(functools.partial(steps, False))

    def planes(first_core):
        return (len(FAR_0), 1) if first_core else (len(FAR_1), len(FAR_1) - 1)

    def in_order(first_core, steps):
        if not first_core:
            return steps((2, 1, 0))
        late = z >= NZ // 2
        pl.when(late)(functools.partial(steps, (0, 1, 2)))
        pl.when(jnp.logical_not(late))(functools.partial(steps, (2, 1, 0)))

    def first_peer(first_core, f):
        if first_core:
            return near[0] + column_0(1, 0)
        return near[0] + column_1(f, 0)

    def first_step(first_core):
        count, each = planes(first_core)
        width = count * each

        def send(h, i):
            k, j = i // each, i % each
            f = 1 if first_core else FAR_1[j]
            remote(
                x_out.at[h, i],
                x_in.at[h, i],
                here_sem.at[3],
                x_sem.at[h, k] if k < count - 1 else recv_sem.at[3],
                first_peer(first_core, f),
            ).start()

        def sums(h, group):
            first, blocks = GROUPS[group]
            k, planes_here = first * count // COLUMN, blocks * count // COLUMN
            outs = planes_here * each
            x_out[h, k * each : k * each + outs] = partial(h, first, outs)
            for i in range(k * each, min(k * each + outs, width - each)):
                send(h, i)

        def keep(h, group):
            first, blocks = GROUPS[group]
            k, planes_here = first * count // COLUMN, blocks * count // COLUMN
            part[h, k : k + planes_here] = partial(h, first + planes_here * each, planes_here)

        wait_rows(0)
        sums(0, NEAREST)
        for group in (1, 0):
            mark_rows(group)
            sums(0, group)
        wait_rows(1)

        def second_half(order):
            for group in order:
                sums(1, group)

        in_order(first_core, second_half)
        for h in range(2):
            for i in range(width - each, width):
                send(h, i)
        for group in (NEAREST, 1, 0):
            for h in range(2):
                keep(h, group)

    by_core(first_step)

    sm_all = all_of(smb.at[0, pl.ds(0, OTHERS)], here_sem.at[2], recv_sem.at[2])
    sm_all.wait_recv()
    for k in (2, 1, 3):
        remote(
            smb.at[0], smb.at[k], here_sem.at[4], recv_sem.at[4], sharers[k]
        ).start()

    def second_step(first_core):
        count, each = planes(first_core)
        half, quarter = count // 2, count // 4
        spans = ((0, quarter), (quarter, half), (half, count - 1))

        def pass_on(h, order):
            for k in [k for group in order for k in range(*spans[group])]:
                arrived = x_in.at[h, pl.ds(k * each, each)]
                all_of(arrived, here_sem.at[3], x_sem.at[h, k]).wait_recv()
                total = part[h, k]
                for j in range(each):
                    total += x_in[h, k * each + j]
                z_out[h, k] = total
                to = column_0(0, FAR_0[k]) if first_core else column_1(0, FAR_1[k])
                remote(
                    z_out.at[h, k],
                    z_in.at[h, k],
                    here_sem.at[5],
                    recv_sem.at[5],
                    near[0] + to,
                ).start()

        pass_on(0, (2, 1, 0))
        in_order(first_core, functools.partial(pass_on, 1))

    by_core(second_step)

    sm_y = all_of(smb.at[pl.ds(1, NEAR - 1)], here_sem.at[4], recv_sem.at[4])
    sm_y.wait_recv()
    count = NEAR * COLUMN * 2
    small = smb[...].reshape(count, 256)
    place = lax.broadcasted_iota(jnp.int32, (examples, count), 1)

    def chosen(values, index):
        result = values[0]
        for i in range(1, len(values)):
            result = jnp.where(index == i, values[i], result)
        return result

    holder = chosen(near, place // (2 * COLUMN)) + chosen(column, lax.rem(place // 2, COLUMN))
    row = holder * 2 + lax.rem(place, 2)
    pick_cols = picks[...].reshape(2, examples).T
    found = [
        jnp.dot(
            jnp.where(pick_cols[:, i : i + 1] == row, 1.0, 0.0).astype(jnp.bfloat16),
            small,
            preferred_element_type=jnp.float32,
        )
        for i in range(2)
    ]
    scaled = dense[...] * found[1]

    def collect(first_core):
        count, each = planes(first_core)
        own = pl.ds((count - 1) * each, each)
        all_of(x_in.at[:, own], here_sem.at[3], recv_sem.at[3]).wait_recv()
        all_of(z_in.at[:, pl.ds(0, count - 1)], here_sem.at[5], recv_sem.at[5]).wait_recv()
        for h in range(2):
            total = part[h, count - 1]
            for j in range(each):
                total += x_in[h, (count - 1) * each + j]
            for k in range(count - 1):
                total += z_in[h, k]
            part[h, 0] = total
        all_of(x_out.at[:, pl.ds(0, count * each)], here_sem.at[3], recv_sem.at[3]).wait_send()
        all_of(z_out.at[:, pl.ds(0, count - 1)], here_sem.at[5], recv_sem.at[5]).wait_send()

    by_core(collect)
    totals = []
    for h in range(2):
        pooled = part[h, 0]
        cut = slice(h * 128, (h + 1) * 128)
        totals.append(scaled[:, cut] + pooled * PICKS ** (-0.5) * found[0][:, cut])
    square = totals[0] * totals[0] + totals[1] * totals[1]
    power = jnp.sum(square, axis=-1, keepdims=True) / 256.0
    inverse = lax.rsqrt(power + 1e-06)
    for h in range(2):
        out_ref[:, h * 128 : (h + 1) * 128] = totals[h] * inverse

    all_of(tab.at[:, pl.ds(1, 3)], here_sem.at[0], y_sem.at[0]).wait_send()
    all_of(idb.at[pl.ds(0, OTHERS)], here_sem.at[1], recv_sem.at[1]).wait_send()
    sm_all.wait_send()
    sm_y.wait_send()


def shards(item_ids, large_table, dense_part, small_ids, small_table, scale_ids):
    examples, features = dense_part.shape
    rows = large_table.shape[0]
    any_space = pl.BlockSpec(memory_space=pl.ANY)
    dma = pltpu.SemaphoreType.DMA
    block = (examples, 128)
    return pl.pallas_call(
        kernel,
        out_shape=pltpu.VMEM((examples, features), jnp.float32),
        in_specs=[any_space] * 6,
        out_specs=pl.BlockSpec(memory_space=pltpu.VMEM),
        scratch_shapes=[
            pltpu.VMEM((2, NEAR, rows, 128), jnp.bfloat16),
            pltpu.VMEM((COLUMN, PICKS, examples), jnp.int32),
            pltpu.VMEM((NEAR, COLUMN, 2, features), jnp.bfloat16),
            pltpu.VMEM((examples, features), jnp.float32),
            pltpu.VMEM((2, 1, examples), jnp.int32),
            pltpu.VMEM((COLUMN * examples, NEAR * rows), jnp.bfloat16),
            pltpu.VMEM((2, 8, *block), jnp.float32),
            pltpu.VMEM((2, 12, *block), jnp.float32),
            pltpu.VMEM((2, 12, *block), jnp.float32),
            pltpu.VMEM((2, 7, *block), jnp.float32),
            pltpu.VMEM((2, 7, *block), jnp.float32),
            dma((6,)),
            dma((6,)),
            dma((2, 7)),
            dma((2,)),
            dma((len(GROUPS),)),
        ],
        compiler_params=pltpu.CompilerParams(collective_id=0, has_side_effects=True),
    )(
        item_ids.T,
        large_table,
        dense_part,
        small_ids.reshape(1, examples),
        scale_ids.reshape(1, examples),
        small_table,
    )


def solution(mesh):
    return jax.shard_map(
        shards,
        mesh=mesh,
        in_specs=(
            P(("ens", "bank"), None),
            P(("ens", "bank"), None),
            P(("ens", "bank"), None),
            P(("ens", "bank")),
            P(("ens", "bank"), None),
            P(("ens", "bank")),
        ),
        out_specs=P(("ens", "bank"), None),
        check_vma=False,
    )
```

```python
import functools

import jax
import jax.numpy as jnp
from jax import lax
from jax.experimental import pallas as pl
from jax.experimental.pallas import tpu as pltpu
from jax.sharding import PartitionSpec as P

PICKS = 2
NZ, NY, NX = 8, 4, 2
NEAR, COLUMN = 4, 16
OTHERS = COLUMN - 1
FAR_0 = (4, 5, 7, 6, 3, 2, 1, 0)
FAR_1 = (2, 3, 1, 0)
COLUMN_0 = [(f, k) for group in (FAR_0[:2], FAR_0[2:4], FAR_0[4:]) for f in (1, 0) for k in group]
COLUMN_1 = [
    pair
    for group in (FAR_1[:1], FAR_1[1:2], FAR_1[2:])
    for pair in [(f, k) for k in group for f in FAR_1[:-1]] + [(0, k) for k in group]
]
GROUPS = ((0, 4), (4, 4), (8, 8))
NEAREST = 2
MESH = pl.DeviceIdType.MESH


def kernel(
    ids_hbm,
    table_hbm,
    dense_hbm,
    small_ids_hbm,
    scale_ids_hbm,
    small_hbm,
    out_ref,
    tab,
    idb,
    smb,
    dense,
    picks,
    onehot,
    part,
    x_out,
    x_in,
    z_out,
    z_in,
    here_sem,
    recv_sem,
    x_sem,
    y_sem,
    ids_sem,
):
    bank = lax.axis_index("bank")
    x = lax.rem(bank, NX)
    y = lax.rem(bank // NX, NY)
    z = bank // (NX * NY)
    second = lax.rem(lax.axis_index("ens"), 2) == 1

    def plan(first_core, second_core):
        return jnp.where(second, second_core, first_core)

    def flip(value, bit):
        return 1 - value if bit else value

    def change(value, bits):
        return sum(flip(lax.rem(value // b, 2), bits // b % 2) * b for b in (1, 2, 4))

    near = [
        plan(
            change(y, k) * NX,
            change(lax.rem(z, 2), k // 2) * (NY * NX) + change(x, k % 2 ^ k // 2),
        )
        for k in range(NEAR)
    ]

    def column_0(f, k):
        return change(x, f) + change(z, k) * (NY * NX)

    def column_1(f, k):
        return change(y, f) * NX + change(z // 2, k) * (2 * NY * NX)

    column = [plan(column_0(*COLUMN_0[i]), column_1(*COLUMN_1[i])) for i in range(COLUMN)]

    def remote(src, dst, send, recv, to):
        return pltpu.make_async_remote_copy(
            src_ref=src,
            dst_ref=dst,
            send_sem=send,
            recv_sem=recv,
            device_id={"bank": to},
            device_id_type=MESH,
        )

    rows = table_hbm.shape[0]
    examples = dense_hbm.shape[0]
    sharers = [near[k] + column[OTHERS] for k in range(NEAR)]
    askers = [near[0] + column[i] for i in range(OTHERS)]

    barrier = pltpu.get_barrier_semaphore()
    for to in askers + sharers[1:]:
        pl.semaphore_signal(barrier, inc=1, device_id={"bank": to}, device_id_type=MESH)

    loads = [
        pltpu.make_async_copy(table_hbm.at[:, pl.ds(0, 128)], tab.at[0, 0], here_sem.at[0]),
        pltpu.make_async_copy(table_hbm.at[:, pl.ds(128, 128)], tab.at[1, 0], here_sem.at[0]),
        pltpu.make_async_copy(ids_hbm, idb.at[OTHERS], here_sem.at[1]),
        pltpu.make_async_copy(small_hbm, smb.at[0, OTHERS], here_sem.at[2]),
        pltpu.make_async_copy(dense_hbm, dense, here_sem.at[3]),
        pltpu.make_async_copy(small_ids_hbm, picks.at[0], here_sem.at[4]),
        pltpu.make_async_copy(scale_ids_hbm, picks.at[1], here_sem.at[4]),
    ]
    for load in loads:
        load.start()
    for buf, i in (
        (tab.at[:, 0], 0), (idb.at[OTHERS], 1), (smb.at[0, OTHERS], 2), (dense, 3), (picks, 4)
    ):
        pltpu.make_async_copy(buf, buf, here_sem.at[i]).wait()
    pl.semaphore_wait(barrier, NEAR - 1 + OTHERS)

    for i in range(OTHERS):
        remote(
            idb.at[OTHERS],
            idb.at[i],
            here_sem.at[1],
            ids_sem.at[min(i // 4, NEAREST)],
            askers[i],
        ).start()
    for i in range(OTHERS):
        remote(
            smb.at[0, OTHERS],
            smb.at[0, i],
            here_sem.at[2],
            recv_sem.at[2],
            askers[i],
        ).start()
    for h in range(2):
        for k in (2, 1, 3):
            remote(
                tab.at[h, 0], tab.at[h, k], here_sem.at[0], y_sem.at[h], sharers[k]
            ).start()
    def all_of(ref, send, recv):
        return remote(ref, ref, send, recv, sharers[1])

    lane = lax.broadcasted_iota(jnp.int32, (examples, 128), 1)

    def mark_rows(group):
        first, blocks = GROUPS[group]
        arrived = idb.at[pl.ds(first, blocks - (group == NEAREST))]
        all_of(arrived, here_sem.at[1], ids_sem.at[group]).wait_recv()
        cols = idb[first : first + blocks].reshape(blocks * PICKS, examples).T
        wide = [
            jnp.broadcast_to(cols[:, c : c + 1], (examples, 128)) for c in range(blocks * PICKS)
        ]
        for k in range(NEAR):
            for cut in range(0, rows, 128):
                here = lane + (sharers[k] * rows + cut)
                for d in range(blocks):
                    once = jnp.where(wide[PICKS * d] == here, 1.0, 0.0)
                    count = jnp.where(wide[PICKS * d + 1] == here, once + 1.0, once)
                    onehot[
                        (first + d) * examples : (first + d + 1) * examples,
                        k * rows + cut : k * rows + cut + 128,
                    ] = count.astype(jnp.bfloat16)

    mark_rows(NEAREST)

    def partial(h, first, blocks):
        total = jnp.dot(
            onehot[first * examples : (first + blocks) * examples, :],
            tab[h].reshape(NEAR * rows, 128),
            preferred_element_type=jnp.float32,
        )
        return total.reshape(blocks, examples, 128)

    def wait_rows(h):
        all_of(tab.at[h, pl.ds(1, NEAR - 1)], here_sem.at[0], y_sem.at[h]).wait_recv()

    def by_core(steps):
        pl.when(jnp.logical_not(second))(functools.partial(steps, True))
        pl.when(second)(functools.partial(steps, False))

    def planes(first_core):
        return (len(FAR_0), 1) if first_core else (len(FAR_1), len(FAR_1) - 1)

    def in_order(first_core, steps):
        if not first_core:
            return steps((2, 1, 0))
        late = z >= NZ // 2
        pl.when(late)(functools.partial(steps, (0, 1, 2)))
        pl.when(jnp.logical_not(late))(functools.partial(steps, (2, 1, 0)))

    def first_peer(first_core, f):
        if first_core:
            return near[0] + column_0(1, 0)
        return near[0] + column_1(f, 0)

    def first_step(first_core):
        count, each = planes(first_core)
        width = count * each

        def group_of(k):
            return min(k * COLUMN // count // 4, NEAREST)

        def send(h, i):
            k, j = i // each, i % each
            f = 1 if first_core else FAR_1[j]
            remote(
                x_out.at[h, i],
                x_in.at[h, i],
                here_sem.at[3],
                x_sem.at[h, group_of(k)] if k < count - 1 else recv_sem.at[3],
                first_peer(first_core, f),
            ).start()

        def sums(h, group):
            first, blocks = GROUPS[group]
            k, planes_here = first * count // COLUMN, blocks * count // COLUMN
            outs = planes_here * each
            x_out[h, k * each : k * each + outs] = partial(h, first, outs)
            for i in range(k * each, min(k * each + outs, width - each)):
                send(h, i)

        def keep(h, group):
            first, blocks = GROUPS[group]
            k, planes_here = first * count // COLUMN, blocks * count // COLUMN
            part[h, k : k + planes_here] = partial(h, first + planes_here * each, planes_here)

        wait_rows(0)
        sums(0, NEAREST)
        for group in (1, 0):
            mark_rows(group)
            sums(0, group)
        wait_rows(1)

        def second_half(order):
            for group in order:
                sums(1, group)

        in_order(first_core, second_half)
        for h in range(2):
            for i in range(width - each, width):
                send(h, i)
        for group in (NEAREST, 1, 0):
            for h in range(2):
                keep(h, group)

    by_core(first_step)

    sm_all = all_of(smb.at[0, pl.ds(0, OTHERS)], here_sem.at[2], recv_sem.at[2])
    sm_all.wait_recv()
    for k in (2, 1, 3):
        remote(
            smb.at[0], smb.at[k], here_sem.at[4], recv_sem.at[4], sharers[k]
        ).start()

    def second_step(first_core):
        count, each = planes(first_core)
        half, quarter = count // 2, count // 4
        spans = ((0, quarter), (quarter, half), (half, count - 1))

        def pass_on(h, order):
            for group in order:
                first, last = spans[group]
                arrived = x_in.at[h, pl.ds(first * each, (last - first) * each)]
                all_of(arrived, here_sem.at[3], x_sem.at[h, group]).wait_recv()
                for k in range(first, last):
                    pass_block(h, k)

        def pass_block(h, k):
            total = part[h, k]
            for j in range(each):
                total += x_in[h, k * each + j]
            z_out[h, k] = total
            to = column_0(0, FAR_0[k]) if first_core else column_1(0, FAR_1[k])
            remote(
                z_out.at[h, k],
                z_in.at[h, k],
                here_sem.at[5],
                recv_sem.at[5],
                near[0] + to,
            ).start()

        pass_on(0, (2, 1, 0))
        in_order(first_core, functools.partial(pass_on, 1))

    by_core(second_step)

    sm_y = all_of(smb.at[pl.ds(1, NEAR - 1)], here_sem.at[4], recv_sem.at[4])
    sm_y.wait_recv()
    count = NEAR * COLUMN * 2
    small = smb[...].reshape(count, 256)
    place = lax.broadcasted_iota(jnp.int32, (examples, count), 1)

    def chosen(values, index):
        result = values[0]
        for i in range(1, len(values)):
            result = jnp.where(index == i, values[i], result)
        return result

    holder = chosen(near, place // (2 * COLUMN)) + chosen(column, lax.rem(place // 2, COLUMN))
    row = holder * 2 + lax.rem(place, 2)
    pick_cols = picks[...].reshape(2, examples).T
    found = [
        jnp.dot(
            jnp.where(pick_cols[:, i : i + 1] == row, 1.0, 0.0).astype(jnp.bfloat16),
            small,
            preferred_element_type=jnp.float32,
        )
        for i in range(2)
    ]
    scaled = dense[...] * found[1]

    def collect(first_core):
        count, each = planes(first_core)
        own = pl.ds((count - 1) * each, each)
        all_of(x_in.at[:, own], here_sem.at[3], recv_sem.at[3]).wait_recv()
        all_of(z_in.at[:, pl.ds(0, count - 1)], here_sem.at[5], recv_sem.at[5]).wait_recv()
        for h in range(2):
            total = part[h, count - 1]
            for j in range(each):
                total += x_in[h, (count - 1) * each + j]
            for k in range(count - 1):
                total += z_in[h, k]
            part[h, 0] = total
        all_of(x_out.at[:, pl.ds(0, count * each)], here_sem.at[3], recv_sem.at[3]).wait_send()
        all_of(z_out.at[:, pl.ds(0, count - 1)], here_sem.at[5], recv_sem.at[5]).wait_send()

    by_core(collect)
    totals = []
    for h in range(2):
        pooled = part[h, 0]
        cut = slice(h * 128, (h + 1) * 128)
        totals.append(scaled[:, cut] + pooled * PICKS ** (-0.5) * found[0][:, cut])
    square = totals[0] * totals[0] + totals[1] * totals[1]
    power = jnp.sum(square, axis=-1, keepdims=True) / 256.0
    inverse = lax.rsqrt(power + 1e-06)
    for h in range(2):
        out_ref[:, h * 128 : (h + 1) * 128] = totals[h] * inverse

    all_of(tab.at[:, pl.ds(1, 3)], here_sem.at[0], y_sem.at[0]).wait_send()
    all_of(idb.at[pl.ds(0, OTHERS)], here_sem.at[1], recv_sem.at[1]).wait_send()
    sm_all.wait_send()
    sm_y.wait_send()


def shards(item_ids, large_table, dense_part, small_ids, small_table, scale_ids):
    examples, features = dense_part.shape
    rows = large_table.shape[0]
    any_space = pl.BlockSpec(memory_space=pl.ANY)
    dma = pltpu.SemaphoreType.DMA
    block = (examples, 128)
    return pl.pallas_call(
        kernel,
        out_shape=pltpu.VMEM((examples, features), jnp.float32),
        in_specs=[any_space] * 6,
        out_specs=pl.BlockSpec(memory_space=pltpu.VMEM),
        scratch_shapes=[
            pltpu.VMEM((2, NEAR, rows, 128), jnp.bfloat16),
            pltpu.VMEM((COLUMN, PICKS, examples), jnp.int32),
            pltpu.VMEM((NEAR, COLUMN, 2, features), jnp.bfloat16),
            pltpu.VMEM((examples, features), jnp.float32),
            pltpu.VMEM((2, 1, examples), jnp.int32),
            pltpu.VMEM((COLUMN * examples, NEAR * rows), jnp.bfloat16),
            pltpu.VMEM((2, 8, *block), jnp.float32),
            pltpu.VMEM((2, 12, *block), jnp.float32),
            pltpu.VMEM((2, 12, *block), jnp.float32),
            pltpu.VMEM((2, 7, *block), jnp.float32),
            pltpu.VMEM((2, 7, *block), jnp.float32),
            dma((6,)),
            dma((6,)),
            dma((2, len(GROUPS))),
            dma((2,)),
            dma((len(GROUPS),)),
        ],
        compiler_params=pltpu.CompilerParams(collective_id=0, has_side_effects=True),
    )(
        item_ids.T,
        large_table,
        dense_part,
        small_ids.reshape(1, examples),
        scale_ids.reshape(1, examples),
        small_table,
    )


def solution(mesh):
    return jax.shard_map(
        shards,
        mesh=mesh,
        in_specs=(
            P(("ens", "bank"), None),
            P(("ens", "bank"), None),
            P(("ens", "bank"), None),
            P(("ens", "bank")),
            P(("ens", "bank"), None),
            P(("ens", "bank")),
        ),
        out_specs=P(("ens", "bank"), None),
        check_vma=False,
    )
```
